32 devices in a mesh: dp: 8 (over z, core), mp: 4 (over y, x).
Axes of the slice: x: 2, y: 2, z: 4, core: 2. Of those that a mesh axis runs over, the one named last changes fastest.
Arguments:
- grad_parts: bfloat16 [8, 64, 256, 256], P('dp', 'mp'), may hold values from -0.25 to 0.25
- left_stats: float32 [8, 4, 4, 256, 256], P('dp', 'mp'), may hold values from -6 to 6
- right_stats: float32 [8, 4, 4, 256, 256], P('dp', 'mp'), may hold values from -6 to 6
- left_root: bfloat16 [8, 4, 4, 256, 256], P('dp', 'mp'), may hold values from -4 to 4
- right_root: bfloat16 [8, 4, 4, 256, 256], P('dp', 'mp'), may hold values from -4 to 4
- owners: int32 [64], replicated, may hold values from 0 to 3, as said below
Outputs:
- direction: bfloat16 [64, 256, 256], P('mp')
- left_updated: float32 [8, 4, 4, 256, 256], P('dp', 'mp')
- right_updated: float32 [8, 4, 4, 256, 256], P('dp', 'mp')
The draws below stay inside these ranges and needn't reach their ends.
Inputs may be any that keep to these rules, and one draw needn't show every extreme that they name: The blocks b with the same b // 2 have distinct owners. Among the blocks of one row, no owner is named more than 4 times, and in every row some owner is named exactly 4 times.
All inputs are finite; a program needn't handle non-finite values.
Results may differ from the reference program's by a relative error of at most 0.02.
Values may be sent and summed in bfloat16 or wider, within the bound.
A program may use at most 64 MiB of HBM per device.

```python
import jax
import jax.numpy as jnp
from jax import lax

B = 256
BD = 2
SLOTS = 4
REPLICAS = 8
OWNERS = 4
NB = 64


def draw_owners(key, part):

    def one_row(row_key):
        key_sigma, key_rank = jax.random.split(row_key, 2)
        sigma = jax.random.permutation(key_sigma, OWNERS).astype(jnp.int32)
        ranks = jax.random.permutation(key_rank, OWNERS).astype(jnp.int32)
        columns = jnp.arange(BD, dtype=jnp.int32)
        classes = ((ranks[:, None] + columns[None, :]) % (OWNERS - 1)).astype(jnp.int32)
        chosen = sigma[1 + classes]
        heavy_holder = (ranks[:, None] < SLOTS) & (columns[None, :] == 0)
        chosen = jnp.where(heavy_holder, sigma[0], chosen)
        return chosen.astype(jnp.int32)
    row_keys = jax.random.split(jax.random.fold_in(key, 7), REPLICAS)
    table = jax.vmap(one_row)(row_keys)
    return jnp.transpose(table, (1, 0, 2)).reshape(NB).astype(jnp.int32)


def block_scale(stream_key, dims, cuts, least, high):
    loudness, own = 1.0, jax.random.fold_in(stream_key, 6)
    for position, parts in cuts:
        heights = jnp.exp(jax.random.uniform(jax.random.fold_in(own, position), (parts,), jnp.float32, least / len(cuts), high / len(cuts)))
        loudness = loudness * jnp.repeat(heights, dims[position] // parts).reshape([-1 if axis == position else 1 for axis in range(len(dims))])
    return loudness


def bell_draw(rng, shape, spread, limit, cuts=(), kind=jnp.bfloat16):
    values = spread * jax.random.normal(rng, shape, jnp.float32)
    if cuts:
        values = values * block_scale(rng, shape, cuts, -0.22, 0.18)
    return jnp.clip(values, -limit, limit).astype(kind)


def setup_inputs(seed: int = 0) -> dict:
    keys = jax.random.split(jax.random.key(seed), 7)
    grad_parts = bell_draw(keys[0], (REPLICAS, NB, B, B), (0.25 / B ** 0.5), 0.25, ((0, 8), (1, 4)))
    left_stats = bell_draw(keys[1], (REPLICAS, OWNERS, SLOTS, B, B), 1.0, 6.0, ((0, 8), (1, 4)), jnp.float32)
    right_stats = bell_draw(keys[2], (REPLICAS, OWNERS, SLOTS, B, B), 1.0, 6.0, ((0, 8), (1, 4)), jnp.float32)
    left_root = bell_draw(keys[3], (REPLICAS, OWNERS, SLOTS, B, B), (B ** -0.25), 4.0, ((0, 8), (1, 4)))
    right_root = bell_draw(keys[4], (REPLICAS, OWNERS, SLOTS, B, B), (B ** -0.25), 4.0, ((0, 8), (1, 4)))
    owners = draw_owners(jax.random.fold_in(keys[6], 71), 0)
    return dict(grad_parts=grad_parts, left_stats=left_stats, right_stats=right_stats, left_root=left_root, right_root=right_root, owners=owners)


def reference(grad_parts, left_stats, right_stats, left_root, right_root, owners):
    def add_part(index, running):
        return running + lax.dynamic_index_in_dim(grad_parts, index, 0, keepdims=False).astype(jnp.float32)

    summed = lax.fori_loop(0, REPLICAS, add_part, jnp.zeros(grad_parts.shape[1:], jnp.float32))
    grad_blocks = summed.astype(jnp.bfloat16)
    block_ids = jnp.arange(NB, dtype=jnp.int32)
    row_of = (block_ids % (BD * REPLICAS)) // BD
    earlier = (row_of[:, None] == row_of[None, :]) & (owners[:, None] == owners[None, :]) & (block_ids[None, :] < block_ids[:, None])
    slot_of = jnp.sum(earlier.astype(jnp.int32), axis=1).astype(jnp.int32)
    slot_key = ((row_of * OWNERS + owners) * SLOTS + slot_of).astype(jnp.int32)
    slot_total = REPLICAS * OWNERS * SLOTS
    source_ids = jnp.zeros((slot_total,), jnp.int32).at[slot_key].set(block_ids)
    filled = jnp.zeros((slot_total,), jnp.int32).at[slot_key].set(jnp.ones((NB,), jnp.int32))
    picked = jnp.take(grad_blocks, source_ids, axis=0)
    owned_grad = jnp.where(filled[:, None, None] > 0, picked, jnp.zeros_like(picked)).astype(jnp.bfloat16)
    left_flat = left_stats.reshape(slot_total, B, B)
    right_flat = right_stats.reshape(slot_total, B, B)
    lroot_flat = left_root.reshape(slot_total, B, B)
    rroot_flat = right_root.reshape(slot_total, B, B)

    def one_slot(items):
        grad_one, left_one, right_one, lroot_one, rroot_one = items
        grad_wide = grad_one.astype(jnp.float32)
        left_next = left_one + jnp.dot(grad_wide, grad_wide.T)
        right_next = right_one + jnp.dot(grad_wide.T, grad_wide)
        half_step = jnp.dot(lroot_one.astype(jnp.float32), grad_wide).astype(jnp.bfloat16)
        result = jnp.dot(half_step.astype(jnp.float32), rroot_one.astype(jnp.float32)).astype(jnp.bfloat16)
        return left_next, right_next, result

    left_next, right_next, precond = lax.map(one_slot, (owned_grad, left_flat, right_flat, lroot_flat, rroot_flat))
    direction = jnp.take(precond, slot_key, axis=0)
    return direction, left_next.reshape(left_stats.shape), right_next.reshape(right_stats.shape)
```

```python
import functools

import jax
import jax.numpy as jnp
from jax import lax
from jax.experimental import pallas as pl
from jax.experimental.pallas import tpu as pltpu
from jax.sharding import PartitionSpec as P

CORES = 2
MESH = pl.DeviceIdType.MESH
F32, BF16 = jnp.float32, jnp.bfloat16


def kernel(
    n, mp, held, slots,
    owners, grads, left_in, right_in, lroot_in, rroot_in,
    dir_out, left_out, right_out,
    own, part, partial, recv, accf, gbuf, pack, arrived, owned, prec, backp, came, dirbuf,
    lstat, rstat, lroot, rroot, back_sel,
    own_sem, part_send, part_recv, red_send, red_recv, fwd_send, fwd_recv, back_send, back_recv,
    gat_send, gat_recv, pair_send, pair_recv, write_sem, stat_sem,
):
    dp, me = lax.axis_index("dp"), lax.axis_index("mp")
    z, c = dp // CORES, dp % CORES
    partner = dp + 1 - 2 * c
    per = n * CORES * held

    def loop(count, body):
        def step(i, carry):
            body(i)
            return carry
        lax.fori_loop(0, count, step, 0)

    def own_copy(d):
        return pltpu.make_async_copy(
            grads.at[0, pl.ds((d * CORES + c) * held, held)],
            own.at[pl.ds(d * held, held)], own_sem.at[d])

    stat_copies = [
        pltpu.make_async_copy(lroot_in.at[0, 0], lroot, stat_sem.at[0]),
        pltpu.make_async_copy(rroot_in.at[0, 0], rroot, stat_sem.at[1]),
        pltpu.make_async_copy(left_in.at[0, 0], lstat, stat_sem.at[2]),
        pltpu.make_async_copy(right_in.at[0, 0], rstat, stat_sem.at[3]),
    ]
    loop(n, lambda d: own_copy(d).start())

    barrier = pltpu.get_barrier_semaphore()
    pl.semaphore_signal(barrier, inc=1, device_id={"dp": partner, "mp": me}, device_id_type=MESH)

    @pl.when(z > 0)
    def _():
        pl.semaphore_signal(barrier, inc=1, device_id={"dp": dp - CORES, "mp": me}, device_id_type=MESH)

    @pl.when(z < n - 1)
    def _():
        pl.semaphore_signal(barrier, inc=1, device_id={"dp": dp + CORES, "mp": me}, device_id_type=MESH)

    for k in range(1, mp):
        pl.semaphore_signal(
            barrier, inc=1, device_id={"dp": dp, "mp": lax.rem(me + k, mp)}, device_id_type=MESH)
    neighbours = jnp.where(z > 0, 1, 0) + jnp.where(z < n - 1, 1, 0)
    pl.semaphore_wait(barrier, mp + neighbours)

    def part_copy(d):
        return pltpu.make_async_remote_copy(
            src_ref=grads.at[0, pl.ds((d * CORES + 1 - c) * held, held)],
            dst_ref=part.at[pl.ds(d * held, held)],
            send_sem=part_send.at[d], recv_sem=part_recv.at[d],
            device_id={"dp": partner, "mp": me}, device_id_type=MESH)

    toward = jnp.where(2 * z < n, 1, -1)

    def far_first(t, sign):
        return jnp.where(sign > 0, n - 1 - t, t)

    loop(n, lambda t: part_copy(far_first(t, toward)).start())
    for copy in stat_copies:
        copy.start()

    def red_copy(d, j, sign, lane):
        i = d * held + j
        return pltpu.make_async_remote_copy(
            src_ref=partial.at[i], dst_ref=recv.at[lane, i],
            send_sem=red_send.at[i], recv_sem=red_recv.at[lane, i],
            device_id={"dp": dp + CORES * sign, "mp": me}, device_id_type=MESH)

    def both(d):
        own_copy(d).wait()
        part_copy(d).wait_recv()

    def red_step(t):
        for stream in range(2):
            sign = toward if stream == 0 else -toward
            lane = jnp.where(sign > 0, 0, 1)
            d = far_first(t, sign)
            before = z - sign

            @pl.when((d - z) * sign > 0)
            def _():
                both(d)

                def block(j):
                    i = d * held + j
                    has = (before >= 0) & (before < n)

                    @pl.when(has)
                    def _():
                        red_copy(d, j, sign, lane).wait_recv()
                        partial[i] = (
                            own[i].astype(F32) + part[i].astype(F32) + recv[lane, i].astype(F32)
                        ).astype(BF16)

                    @pl.when(jnp.logical_not(has))
                    def _():
                        partial[i] = (own[i].astype(F32) + part[i].astype(F32)).astype(BF16)

                    red_copy(d, j, sign, lane).start()

                loop(held, block)

    loop(n - 1, red_step)

    my_owner = [owners[me * per + dp * held + j] for j in range(held)]

    def held_for(q):
        pick = jnp.int32(0)
        for j in range(held):
            pick = jnp.where(my_owner[j] == q, j, pick)
        return pick

    count = jnp.int32(0)
    source = [jnp.int32(0)] * slots
    filled = [jnp.int32(0)] * slots
    for q in range(mp):
        slot_for_q = jnp.int32(0)
        for j in range(held):
            mine = owners[q * per + dp * held + j] == me
            for s in range(slots):
                hit = mine & (count == s)
                source[s] = jnp.where(hit, q, source[s])
                filled[s] = jnp.where(hit, 1, filled[s])
                slot_for_q = jnp.where(hit, s, slot_for_q)
            count = count + mine.astype(jnp.int32)
        back_sel[q] = slot_for_q

    both(z)

    def finish(j):
        i = z * held + j
        accf[...] = own[i].astype(F32) + part[i].astype(F32)

        @pl.when(z > 0)
        def _():
            red_copy(z, j, 1, 0).wait_recv()
            accf[...] += recv[0, i].astype(F32)

        @pl.when(z < n - 1)
        def _():
            red_copy(z, j, -1, 1).wait_recv()
            accf[...] += recv[1, i].astype(F32)

        gbuf[j] = accf[...].astype(BF16)

    loop(held, finish)

    def exchange(src, dst, sends, recvs, k):
        return pltpu.make_async_remote_copy(
            src_ref=src.at[k], dst_ref=dst.at[me],
            send_sem=sends.at[k], recv_sem=recvs.at[k],
            device_id={"dp": dp, "mp": lax.rem(me + k, mp)}, device_id_type=MESH)

    def send_held(t):
        k = mp - 1 - t
        pack[k] = gbuf[held_for(lax.rem(me + k, mp))]
        exchange(pack, arrived, fwd_send, fwd_recv, k).start()

    loop(mp - 1, send_held)
    arrived[me] = gbuf[held_for(me)]
    for copy in stat_copies[:2]:
        copy.wait()
    loop(mp - 1, lambda t: exchange(pack, arrived, fwd_send, fwd_recv, t + 1).wait_recv())

    def dot(a, b, dims=((1,), (0,))):
        return lax.dot_general(a, b, (dims, ((), ())), preferred_element_type=F32)

    for s in range(slots):
        block = arrived[source[s]]
        owned[s] = jnp.where(filled[s] > 0, block.astype(F32), 0.0).astype(BF16)
    for s in range(slots):
        half = dot(lroot[s], owned[s]).astype(BF16)
        prec[s] = dot(half, rroot[s]).astype(BF16)

    def send_back(t):
        k = mp - 1 - t
        backp[k] = prec[back_sel[lax.rem(me + k, mp)]]
        exchange(backp, came, back_send, back_recv, k).start()

    loop(mp - 1, send_back)
    came[me] = prec[back_sel[me]]

    for copy in stat_copies[2:]:
        copy.wait()
    for s in range(slots):
        lstat[s] += dot(owned[s], owned[s], ((1,), (1,)))
        rstat[s] += dot(owned[s], owned[s], ((0,), (0,)))
    stat_writes = [
        pltpu.make_async_copy(lstat, left_out.at[0, 0], stat_sem.at[4]),
        pltpu.make_async_copy(rstat, right_out.at[0, 0], stat_sem.at[5]),
    ]
    for copy in stat_writes:
        copy.start()
    loop(mp - 1, lambda t: exchange(backp, came, back_send, back_recv, t + 1).wait_recv())
    for j in range(held):
        dirbuf[dp * held + j] = came[my_owner[j]]

    def gat_copy(r, j, sign, lane):
        i = (r * CORES + c) * held + j
        return pltpu.make_async_remote_copy(
            src_ref=dirbuf.at[i], dst_ref=dirbuf.at[i],
            send_sem=gat_send.at[lane, r * held + j], recv_sem=gat_recv.at[r * held + j],
            device_id={"dp": dp + CORES * sign, "mp": me}, device_id_type=MESH)

    def pair_copy(r, j, core):
        i = (r * CORES + core) * held + j
        return pltpu.make_async_remote_copy(
            src_ref=dirbuf.at[i], dst_ref=dirbuf.at[i],
            send_sem=pair_send.at[r * held + j], recv_sem=pair_recv.at[r * held + j],
            device_id={"dp": partner, "mp": me}, device_id_type=MESH)

    def write(r, core):
        i = (r * CORES + core) * held
        return pltpu.make_async_copy(
            dirbuf.at[pl.ds(i, held)], dir_out.at[pl.ds(i, held)],
            write_sem.at[r * CORES + core])

    def first(j):
        @pl.when(z < n - 1)
        def _():
            gat_copy(z, j, 1, 0).start()

        @pl.when(z > 0)
        def _():
            gat_copy(z, j, -1, 1).start()

        pair_copy(z, j, c).start()

    loop(held, first)
    write(z, c).start()

    def gather_step(t):
        for lane, sign in ((0, 1), (1, -1)):
            r = z - sign * (t + 1)
            after = z + sign

            @pl.when((r >= 0) & (r < n))
            def _():
                def block(j):
                    gat_copy(r, j, sign, lane).wait_recv()

                    @pl.when((after >= 0) & (after < n))
                    def _():
                        gat_copy(r, j, sign, lane).start()

                    pair_copy(r, j, c).start()

                loop(held, block)
                write(r, c).start()

    loop(n - 1, gather_step)

    def pair_row(r):
        loop(held, lambda j: pair_copy(r, j, 1 - c).wait_recv())
        write(r, 1 - c).start()

    pair_row(z)

    def pair_step(t):
        for sign in (1, -1):
            r = z - sign * (t + 1)

            @pl.when((r >= 0) & (r < n))
            def _():
                pair_row(r)

    loop(n - 1, pair_step)

    def drain(r):
        part_copy(r).wait_send()
        write(r, 0).wait()
        write(r, 1).wait()

        def block(j):
            pair_copy(r, j, c).wait_send()

            @pl.when(r != z)
            def _():
                red_copy(r, j, 1, 0).wait_send()

            @pl.when((r <= z) & (z < n - 1))
            def _():
                gat_copy(r, j, 1, 0).wait_send()

            @pl.when((r >= z) & (z > 0))
            def _():
                gat_copy(r, j, -1, 1).wait_send()

        loop(held, block)

    loop(n, drain)

    def drain_exchange(t):
        exchange(pack, arrived, fwd_send, fwd_recv, t + 1).wait_send()
        exchange(backp, came, back_send, back_recv, t + 1).wait_send()

    loop(mp - 1, drain_exchange)
    for copy in stat_writes:
        copy.wait()


def per_device(n_dp, mp, grad_parts, left_stats, right_stats, left_root, right_root, owners):
    n = n_dp // CORES
    per, (rows, cols) = grad_parts.shape[1], grad_parts.shape[2:]
    held, slots = per // n_dp, left_stats.shape[2]
    hbm = pl.BlockSpec(memory_space=pltpu.HBM)

    def blocks(*lead, kind=BF16):
        return pltpu.VMEM((*lead, rows, cols), kind)

    dma = pltpu.SemaphoreType.DMA
    return pl.pallas_call(
        functools.partial(kernel, n, mp, held, slots),
        out_shape=(
            jax.ShapeDtypeStruct((per, rows, cols), BF16),
            jax.ShapeDtypeStruct(left_stats.shape, F32),
            jax.ShapeDtypeStruct(right_stats.shape, F32),
        ),
        in_specs=[pl.BlockSpec(memory_space=pltpu.SMEM)] + [hbm] * 5,
        out_specs=(hbm, hbm, hbm),
        scratch_shapes=[
            blocks(n * held), blocks(n * held), blocks(n * held), blocks(2, n * held),
            blocks(kind=F32), blocks(held), blocks(mp), blocks(mp), blocks(slots), blocks(slots),
            blocks(mp), blocks(mp), blocks(per),
            blocks(slots, kind=F32), blocks(slots, kind=F32), blocks(slots), blocks(slots),
            pltpu.SMEM((mp,), jnp.int32),
            dma((n,)), dma((n,)), dma((n,)), dma((n * held,)), dma((2, n * held)),
            dma((mp,)), dma((mp,)), dma((mp,)), dma((mp,)),
            dma((2, n * held)), dma((n * held,)), dma((n * held,)), dma((n * held,)),
            dma((n_dp,)), dma((6,)),
        ],
        compiler_params=pltpu.CompilerParams(
            collective_id=0, has_side_effects=True),
    )(owners, grad_parts, left_stats, right_stats, left_root, right_root)


def solution(mesh):
    five = P("dp", "mp", None, None, None)
    return jax.shard_map(
        functools.partial(per_device, mesh.shape["dp"], mesh.shape["mp"]),
        mesh=mesh,
        in_specs=(P("dp", "mp", None, None), five, five, five, five, P()),
        out_specs=(P("mp", None, None), five, five),
        check_vma=False,
    )
```

```python
import functools

import jax
import jax.numpy as jnp
from jax import lax
from jax.experimental import pallas as pl
from jax.experimental.pallas import tpu as pltpu
from jax.sharding import PartitionSpec as P

CORES = 2
MESH = pl.DeviceIdType.MESH
F32, BF16 = jnp.float32, jnp.bfloat16


def kernel(
    n, mp, held, slots,
    owners, grads, left_in, right_in, lroot_in, rroot_in,
    dir_out, left_out, right_out,
    own, part, partial, recv, accf, gbuf, pack, arrived, owned, prec, backp, came, dirbuf,
    lstat, rstat, lroot, rroot, back_sel,
    own_sem, part_send, part_recv, red_send, red_recv, fwd_send, fwd_recv, back_send, back_recv,
    gat_send, gat_recv, pair_send, pair_recv, write_sem, stat_sem, turn_sem,
):
    dp, me = lax.axis_index("dp"), lax.axis_index("mp")
    z, c = dp // CORES, dp % CORES
    partner = dp + 1 - 2 * c
    per = n * CORES * held

    def loop(count, body):
        def step(i, carry):
            body(i)
            return carry
        lax.fori_loop(0, count, step, 0)

    def own_copy(d):
        return pltpu.make_async_copy(
            grads.at[0, pl.ds((d * CORES + c) * held, held)],
            own.at[pl.ds(d * held, held)], own_sem.at[d])

    stat_copies = [
        pltpu.make_async_copy(lroot_in.at[0, 0], lroot, stat_sem.at[0]),
        pltpu.make_async_copy(rroot_in.at[0, 0], rroot, stat_sem.at[1]),
        pltpu.make_async_copy(left_in.at[0, 0], lstat, stat_sem.at[2]),
        pltpu.make_async_copy(right_in.at[0, 0], rstat, stat_sem.at[3]),
    ]
    loop(n, lambda d: own_copy(d).start())

    barrier = pltpu.get_barrier_semaphore()
    pl.semaphore_signal(barrier, inc=1, device_id={"dp": partner, "mp": me}, device_id_type=MESH)

    @pl.when(z > 0)
    def _():
        pl.semaphore_signal(barrier, inc=1, device_id={"dp": dp - CORES, "mp": me}, device_id_type=MESH)

    @pl.when(z < n - 1)
    def _():
        pl.semaphore_signal(barrier, inc=1, device_id={"dp": dp + CORES, "mp": me}, device_id_type=MESH)

    for k in range(1, mp):
        pl.semaphore_signal(
            barrier, inc=1, device_id={"dp": dp, "mp": lax.rem(me + k, mp)}, device_id_type=MESH)
    neighbours = jnp.where(z > 0, 1, 0) + jnp.where(z < n - 1, 1, 0)
    pl.semaphore_wait(barrier, mp + neighbours)

    def part_copy(d):
        return pltpu.make_async_remote_copy(
            src_ref=grads.at[0, pl.ds((d * CORES + 1 - c) * held, held)],
            dst_ref=part.at[pl.ds(d * held, held)],
            send_sem=part_send.at[d], recv_sem=part_recv.at[d],
            device_id={"dp": partner, "mp": me}, device_id_type=MESH)

    toward = jnp.where(2 * z < n, 1, -1)

    def far_first(t, sign):
        return jnp.where(sign > 0, n - 1 - t, t)

    loop(n, lambda t: part_copy(far_first(t, toward)).start())
    for copy in stat_copies:
        copy.start()

    def red_copy(d, j, sign, lane):
        i = d * held + j
        return pltpu.make_async_remote_copy(
            src_ref=partial.at[i], dst_ref=recv.at[lane, i],
            send_sem=red_send.at[i], recv_sem=red_recv.at[lane, i],
            device_id={"dp": dp + CORES * sign, "mp": me}, device_id_type=MESH)

    def both(d):
        own_copy(d).wait()
        part_copy(d).wait_recv()

    def red_step(t):
        for stream in range(2):
            sign = toward if stream == 0 else -toward
            lane = jnp.where(sign > 0, 0, 1)
            d = far_first(t, sign)
            before = z - sign

            @pl.when((d - z) * sign > 0)
            def _():
                both(d)

                def block(j):
                    i = d * held + j
                    has = (before >= 0) & (before < n)

                    @pl.when(has)
                    def _():
                        red_copy(d, j, sign, lane).wait_recv()
                        partial[i] = (
                            own[i].astype(F32) + part[i].astype(F32) + recv[lane, i].astype(F32)
                        ).astype(BF16)

                    @pl.when(jnp.logical_not(has))
                    def _():
                        partial[i] = (own[i].astype(F32) + part[i].astype(F32)).astype(BF16)

                    red_copy(d, j, sign, lane).start()

                loop(held, block)

    @pl.when(c == 1)
    def _():
        pl.semaphore_wait(turn_sem, 1)

    loop(n - 1, red_step)

    def sums_left(d):
        @pl.when(d != z)
        def _():
            loop(held, lambda j: red_copy(d, j, 1, 0).wait_send())

    @pl.when(c == 0)
    def _():
        loop(n, sums_left)
        pl.semaphore_signal(
            turn_sem, inc=1, device_id={"dp": partner, "mp": me}, device_id_type=MESH)

    my_owner = [owners[me * per + dp * held + j] for j in range(held)]

    def held_for(q):
        pick = jnp.int32(0)
        for j in range(held):
            pick = jnp.where(my_owner[j] == q, j, pick)
        return pick

    count = jnp.int32(0)
    source = [jnp.int32(0)] * slots
    filled = [jnp.int32(0)] * slots
    for q in range(mp):
        slot_for_q = jnp.int32(0)
        for j in range(held):
            mine = owners[q * per + dp * held + j] == me
            for s in range(slots):
                hit = mine & (count == s)
                source[s] = jnp.where(hit, q, source[s])
                filled[s] = jnp.where(hit, 1, filled[s])
                slot_for_q = jnp.where(hit, s, slot_for_q)
            count = count + mine.astype(jnp.int32)
        back_sel[q] = slot_for_q

    both(z)

    def finish(j):
        i = z * held + j
        accf[...] = own[i].astype(F32) + part[i].astype(F32)

        @pl.when(z > 0)
        def _():
            red_copy(z, j, 1, 0).wait_recv()
            accf[...] += recv[0, i].astype(F32)

        @pl.when(z < n - 1)
        def _():
            red_copy(z, j, -1, 1).wait_recv()
            accf[...] += recv[1, i].astype(F32)

        gbuf[j] = accf[...].astype(BF16)

    loop(held, finish)

    def exchange(src, dst, sends, recvs, k):
        return pltpu.make_async_remote_copy(
            src_ref=src.at[k], dst_ref=dst.at[me],
            send_sem=sends.at[k], recv_sem=recvs.at[k],
            device_id={"dp": dp, "mp": lax.rem(me + k, mp)}, device_id_type=MESH)

    def send_held(t):
        k = mp - 1 - t
        pack[k] = gbuf[held_for(lax.rem(me + k, mp))]
        exchange(pack, arrived, fwd_send, fwd_recv, k).start()

    loop(mp - 1, send_held)
    arrived[me] = gbuf[held_for(me)]
    for copy in stat_copies[:2]:
        copy.wait()
    loop(mp - 1, lambda t: exchange(pack, arrived, fwd_send, fwd_recv, t + 1).wait_recv())

    def dot(a, b, dims=((1,), (0,))):
        return lax.dot_general(a, b, (dims, ((), ())), preferred_element_type=F32)

    for s in range(slots):
        block = arrived[source[s]]
        owned[s] = jnp.where(filled[s] > 0, block.astype(F32), 0.0).astype(BF16)
    for s in range(slots):
        half = dot(lroot[s], owned[s]).astype(BF16)
        prec[s] = dot(half, rroot[s]).astype(BF16)

    def send_back(t):
        k = mp - 1 - t
        backp[k] = prec[back_sel[lax.rem(me + k, mp)]]
        exchange(backp, came, back_send, back_recv, k).start()

    loop(mp - 1, send_back)
    came[me] = prec[back_sel[me]]

    for copy in stat_copies[2:]:
        copy.wait()
    for s in range(slots):
        lstat[s] += dot(owned[s], owned[s], ((1,), (1,)))
        rstat[s] += dot(owned[s], owned[s], ((0,), (0,)))
    stat_writes = [
        pltpu.make_async_copy(lstat, left_out.at[0, 0], stat_sem.at[4]),
        pltpu.make_async_copy(rstat, right_out.at[0, 0], stat_sem.at[5]),
    ]
    for copy in stat_writes:
        copy.start()
    loop(mp - 1, lambda t: exchange(backp, came, back_send, back_recv, t + 1).wait_recv())
    for j in range(held):
        dirbuf[dp * held + j] = came[my_owner[j]]

    def gat_copy(r, j, sign, lane):
        i = (r * CORES + c) * held + j
        return pltpu.make_async_remote_copy(
            src_ref=dirbuf.at[i], dst_ref=dirbuf.at[i],
            send_sem=gat_send.at[lane, r * held + j], recv_sem=gat_recv.at[r * held + j],
            device_id={"dp": dp + CORES * sign, "mp": me}, device_id_type=MESH)

    def pair_copy(r, j, core):
        i = (r * CORES + core) * held + j
        return pltpu.make_async_remote_copy(
            src_ref=dirbuf.at[i], dst_ref=dirbuf.at[i],
            send_sem=pair_send.at[r * held + j], recv_sem=pair_recv.at[r * held + j],
            device_id={"dp": partner, "mp": me}, device_id_type=MESH)

    def write(r, core):
        i = (r * CORES + core) * held
        return pltpu.make_async_copy(
            dirbuf.at[pl.ds(i, held)], dir_out.at[pl.ds(i, held)],
            write_sem.at[r * CORES + core])

    def first(j):
        @pl.when(z < n - 1)
        def _():
            gat_copy(z, j, 1, 0).start()

        @pl.when(z > 0)
        def _():
            gat_copy(z, j, -1, 1).start()

        pair_copy(z, j, c).start()

    loop(held, first)
    write(z, c).start()

    def gather_step(t):
        for lane, sign in ((0, 1), (1, -1)):
            r = z - sign * (t + 1)
            after = z + sign

            @pl.when((r >= 0) & (r < n))
            def _():
                def block(j):
                    gat_copy(r, j, sign, lane).wait_recv()

                    @pl.when((after >= 0) & (after < n))
                    def _():
                        gat_copy(r, j, sign, lane).start()

                    pair_copy(r, j, c).start()

                loop(held, block)
                write(r, c).start()

    loop(n - 1, gather_step)

    def pair_row(r):
        loop(held, lambda j: pair_copy(r, j, 1 - c).wait_recv())
        write(r, 1 - c).start()

    pair_row(z)

    def pair_step(t):
        for sign in (1, -1):
            r = z - sign * (t + 1)

            @pl.when((r >= 0) & (r < n))
            def _():
                pair_row(r)

    loop(n - 1, pair_step)

    def drain(r):
        part_copy(r).wait_send()
        write(r, 0).wait()
        write(r, 1).wait()

        def block(j):
            pair_copy(r, j, c).wait_send()

            @pl.when((r != z) & (c == 1))
            def _():
                red_copy(r, j, 1, 0).wait_send()

            @pl.when((r <= z) & (z < n - 1))
            def _():
                gat_copy(r, j, 1, 0).wait_send()

            @pl.when((r >= z) & (z > 0))
            def _():
                gat_copy(r, j, -1, 1).wait_send()

        loop(held, block)

    loop(n, drain)

    def drain_exchange(t):
        exchange(pack, arrived, fwd_send, fwd_recv, t + 1).wait_send()
        exchange(backp, came, back_send, back_recv, t + 1).wait_send()

    loop(mp - 1, drain_exchange)
    for copy in stat_writes:
        copy.wait()


def per_device(n_dp, mp, grad_parts, left_stats, right_stats, left_root, right_root, owners):
    n = n_dp // CORES
    per, (rows, cols) = grad_parts.shape[1], grad_parts.shape[2:]
    held, slots = per // n_dp, left_stats.shape[2]
    hbm = pl.BlockSpec(memory_space=pltpu.HBM)

    def blocks(*lead, kind=BF16):
        return pltpu.VMEM((*lead, rows, cols), kind)

    dma = pltpu.SemaphoreType.DMA
    return pl.pallas_call(
        functools.partial(kernel, n, mp, held, slots),
        out_shape=(
            jax.ShapeDtypeStruct((per, rows, cols), BF16),
            jax.ShapeDtypeStruct(left_stats.shape, F32),
            jax.ShapeDtypeStruct(right_stats.shape, F32),
        ),
        in_specs=[pl.BlockSpec(memory_space=pltpu.SMEM)] + [hbm] * 5,
        out_specs=(hbm, hbm, hbm),
        scratch_shapes=[
            blocks(n * held), blocks(n * held), blocks(n * held), blocks(2, n * held),
            blocks(kind=F32), blocks(held), blocks(mp), blocks(mp), blocks(slots), blocks(slots),
            blocks(mp), blocks(mp), blocks(per),
            blocks(slots, kind=F32), blocks(slots, kind=F32), blocks(slots), blocks(slots),
            pltpu.SMEM((mp,), jnp.int32),
            dma((n,)), dma((n,)), dma((n,)), dma((n * held,)), dma((2, n * held)),
            dma((mp,)), dma((mp,)), dma((mp,)), dma((mp,)),
            dma((2, n * held)), dma((n * held,)), dma((n * held,)), dma((n * held,)),
            dma((n_dp,)), dma((6,)), pltpu.SemaphoreType.REGULAR,
        ],
        compiler_params=pltpu.CompilerParams(
            collective_id=0, has_side_effects=True),
    )(owners, grad_parts, left_stats, right_stats, left_root, right_root)


def solution(mesh):
    five = P("dp", "mp", None, None, None)
    return jax.shard_map(
        functools.partial(per_device, mesh.shape["dp"], mesh.shape["mp"]),
        mesh=mesh,
        in_specs=(P("dp", "mp", None, None), five, five, five, five, P()),
        out_specs=(P("mp", None, None), five, five),
        check_vma=False,
    )
```

```python
import functools

import jax
import jax.numpy as jnp
from jax import lax
from jax.experimental import pallas as pl
from jax.experimental.pallas import tpu as pltpu
from jax.sharding import PartitionSpec as P

CORES = 2
MESH = pl.DeviceIdType.MESH
F32, BF16 = jnp.float32, jnp.bfloat16


def kernel(
    n, mp, held, slots,
    owners_in, grads, left_in, right_in, lroot_in, rroot_in,
    dirbuf, lstat, rstat,
    own, part, partial, recv, accf, gbuf, pack, arrived, owned, prec, backp, came,
    lroot, rroot, owners, back_sel,
    own_sem, part_send, part_recv, red_send, red_recv, fwd_send, fwd_recv, back_send, back_recv,
    gat_send, gat_recv, pair_send, pair_recv, stat_sem, turn_sem,
):
    dp, me = lax.axis_index("dp"), lax.axis_index("mp")
    z, c = dp // CORES, dp % CORES
    partner = dp + 1 - 2 * c
    per = n * CORES * held

    def loop(count, body):
        def step(i, carry):
            body(i)
            return carry
        lax.fori_loop(0, count, step, 0)

    def own_copy(d):
        return pltpu.make_async_copy(
            grads.at[0, pl.ds((d * CORES + c) * held, held)],
            own.at[pl.ds(d * held, held)], own_sem.at[d])

    stat_copies = [
        pltpu.make_async_copy(lroot_in.at[0, 0], lroot, stat_sem.at[0]),
        pltpu.make_async_copy(rroot_in.at[0, 0], rroot, stat_sem.at[1]),
        pltpu.make_async_copy(left_in, lstat, stat_sem.at[2]),
        pltpu.make_async_copy(right_in, rstat, stat_sem.at[3]),
    ]
    owners_copy = pltpu.make_async_copy(owners_in, owners, stat_sem.at[4])
    owners_copy.start()
    loop(n, lambda d: own_copy(d).start())

    barrier = pltpu.get_barrier_semaphore()
    pl.semaphore_signal(barrier, inc=1, device_id={"dp": partner, "mp": me}, device_id_type=MESH)

    @pl.when(z > 0)
    def _():
        pl.semaphore_signal(barrier, inc=1, device_id={"dp": dp - CORES, "mp": me}, device_id_type=MESH)

    @pl.when(z < n - 1)
    def _():
        pl.semaphore_signal(barrier, inc=1, device_id={"dp": dp + CORES, "mp": me}, device_id_type=MESH)

    for k in range(1, mp):
        pl.semaphore_signal(
            barrier, inc=1, device_id={"dp": dp, "mp": lax.rem(me + k, mp)}, device_id_type=MESH)
    neighbours = jnp.where(z > 0, 1, 0) + jnp.where(z < n - 1, 1, 0)
    pl.semaphore_wait(barrier, mp + neighbours)

    def part_copy(d):
        return pltpu.make_async_remote_copy(
            src_ref=grads.at[0, pl.ds((d * CORES + 1 - c) * held, held)],
            dst_ref=part.at[pl.ds(d * held, held)],
            send_sem=part_send.at[d], recv_sem=part_recv.at[d],
            device_id={"dp": partner, "mp": me}, device_id_type=MESH)

    toward = jnp.where(2 * z < n, 1, -1)

    def far_first(t, sign):
        return jnp.where(sign > 0, n - 1 - t, t)

    loop(n, lambda t: part_copy(far_first(t, toward)).start())
    for copy in stat_copies:
        copy.start()

    def red_copy(d, j, sign, lane):
        i = d * held + j
        return pltpu.make_async_remote_copy(
            src_ref=partial.at[i], dst_ref=recv.at[lane, i],
            send_sem=red_send.at[i], recv_sem=red_recv.at[lane, i],
            device_id={"dp": dp + CORES * sign, "mp": me}, device_id_type=MESH)

    def both(d):
        own_copy(d).wait()
        part_copy(d).wait_recv()

    def red_step(t):
        for stream in range(2):
            sign = toward if stream == 0 else -toward
            lane = jnp.where(sign > 0, 0, 1)
            d = far_first(t, sign)
            before = z - sign

            @pl.when((d - z) * sign > 0)
            def _():
                both(d)

                def block(j):
                    i = d * held + j
                    has = (before >= 0) & (before < n)

                    @pl.when(has)
                    def _():
                        red_copy(d, j, sign, lane).wait_recv()
                        partial[i] = (
                            own[i].astype(F32) + part[i].astype(F32) + recv[lane, i].astype(F32)
                        ).astype(BF16)

                    @pl.when(jnp.logical_not(has))
                    def _():
                        partial[i] = (own[i].astype(F32) + part[i].astype(F32)).astype(BF16)

                    red_copy(d, j, sign, lane).start()

                loop(held, block)

    @pl.when(c == 1)
    def _():
        pl.semaphore_wait(turn_sem, 1)

    loop(n - 1, red_step)

    def sums_left(d):
        @pl.when(d != z)
        def _():
            loop(held, lambda j: red_copy(d, j, 1, 0).wait_send())

    @pl.when(c == 0)
    def _():
        loop(n, sums_left)
        pl.semaphore_signal(
            turn_sem, inc=1, device_id={"dp": partner, "mp": me}, device_id_type=MESH)

    owners_copy.wait()
    my_owner = [owners[me * per + dp * held + j] for j in range(held)]

    def held_for(q):
        pick = jnp.int32(0)
        for j in range(held):
            pick = jnp.where(my_owner[j] == q, j, pick)
        return pick

    count = jnp.int32(0)
    source = [jnp.int32(0)] * slots
    filled = [jnp.int32(0)] * slots
    for q in range(mp):
        slot_for_q = jnp.int32(0)
        for j in range(held):
            mine = owners[q * per + dp * held + j] == me
            for s in range(slots):
                hit = mine & (count == s)
                source[s] = jnp.where(hit, q, source[s])
                filled[s] = jnp.where(hit, 1, filled[s])
                slot_for_q = jnp.where(hit, s, slot_for_q)
            count = count + mine.astype(jnp.int32)
        back_sel[q] = slot_for_q

    both(z)

    def finish(j):
        i = z * held + j
        accf[...] = own[i].astype(F32) + part[i].astype(F32)

        @pl.when(z > 0)
        def _():
            red_copy(z, j, 1, 0).wait_recv()
            accf[...] += recv[0, i].astype(F32)

        @pl.when(z < n - 1)
        def _():
            red_copy(z, j, -1, 1).wait_recv()
            accf[...] += recv[1, i].astype(F32)

        gbuf[j] = accf[...].astype(BF16)

    loop(held, finish)

    def exchange(src, dst, sends, recvs, k):
        return pltpu.make_async_remote_copy(
            src_ref=src.at[k], dst_ref=dst.at[me],
            send_sem=sends.at[k], recv_sem=recvs.at[k],
            device_id={"dp": dp, "mp": lax.rem(me + k, mp)}, device_id_type=MESH)

    def send_held(t):
        k = mp - 1 - t
        pack[k] = gbuf[held_for(lax.rem(me + k, mp))]
        exchange(pack, arrived, fwd_send, fwd_recv, k).start()

    loop(mp - 1, send_held)
    arrived[me] = gbuf[held_for(me)]
    for copy in stat_copies[:2]:
        copy.wait()
    loop(mp - 1, lambda t: exchange(pack, arrived, fwd_send, fwd_recv, t + 1).wait_recv())

    def dot(a, b, dims=((1,), (0,))):
        return lax.dot_general(a, b, (dims, ((), ())), preferred_element_type=F32)

    for s in range(slots):
        block = arrived[source[s]]
        owned[s] = jnp.where(filled[s] > 0, block.astype(F32), 0.0).astype(BF16)
    for s in range(slots):
        half = dot(lroot[s], owned[s]).astype(BF16)
        prec[s] = dot(half, rroot[s]).astype(BF16)

    def send_back(t):
        k = mp - 1 - t
        backp[k] = prec[back_sel[lax.rem(me + k, mp)]]
        exchange(backp, came, back_send, back_recv, k).start()

    loop(mp - 1, send_back)
    came[me] = prec[back_sel[me]]

    for copy in stat_copies[2:]:
        copy.wait()
    for s in range(slots):
        lstat[0, 0, s] += dot(owned[s], owned[s], ((1,), (1,)))
        rstat[0, 0, s] += dot(owned[s], owned[s], ((0,), (0,)))
    loop(mp - 1, lambda t: exchange(backp, came, back_send, back_recv, t + 1).wait_recv())
    for j in range(held):
        dirbuf[dp * held + j] = came[my_owner[j]]

    def gat_copy(r, j, sign, lane):
        i = (r * CORES + c) * held + j
        return pltpu.make_async_remote_copy(
            src_ref=dirbuf.at[i], dst_ref=dirbuf.at[i],
            send_sem=gat_send.at[lane, r * held + j], recv_sem=gat_recv.at[r * held + j],
            device_id={"dp": dp + CORES * sign, "mp": me}, device_id_type=MESH)

    def pair_copy(r, j, core):
        i = (r * CORES + core) * held + j
        return pltpu.make_async_remote_copy(
            src_ref=dirbuf.at[i], dst_ref=dirbuf.at[i],
            send_sem=pair_send.at[r * held + j], recv_sem=pair_recv.at[r * held + j],
            device_id={"dp": partner, "mp": me}, device_id_type=MESH)

    def first(j):
        @pl.when(z < n - 1)
        def _():
            gat_copy(z, j, 1, 0).start()

        @pl.when(z > 0)
        def _():
            gat_copy(z, j, -1, 1).start()

        pair_copy(z, j, c).start()

    loop(held, first)

    def gather_step(t):
        for lane, sign in ((0, 1), (1, -1)):
            r = z - sign * (t + 1)
            after = z + sign

            @pl.when((r >= 0) & (r < n))
            def _():
                def block(j):
                    gat_copy(r, j, sign, lane).wait_recv()

                    @pl.when((after >= 0) & (after < n))
                    def _():
                        gat_copy(r, j, sign, lane).start()

                    pair_copy(r, j, c).start()

                loop(held, block)

    loop(n - 1, gather_step)

    def pair_row(r):
        loop(held, lambda j: pair_copy(r, j, 1 - c).wait_recv())

    pair_row(z)

    def pair_step(t):
        for sign in (1, -1):
            r = z - sign * (t + 1)

            @pl.when((r >= 0) & (r < n))
            def _():
                pair_row(r)

    loop(n - 1, pair_step)

    def drain(r):
        part_copy(r).wait_send()

        def block(j):
            pair_copy(r, j, c).wait_send()

            @pl.when((r != z) & (c == 1))
            def _():
                red_copy(r, j, 1, 0).wait_send()

            @pl.when((r <= z) & (z < n - 1))
            def _():
                gat_copy(r, j, 1, 0).wait_send()

            @pl.when((r >= z) & (z > 0))
            def _():
                gat_copy(r, j, -1, 1).wait_send()

        loop(held, block)

    loop(n, drain)

    def drain_exchange(t):
        exchange(pack, arrived, fwd_send, fwd_recv, t + 1).wait_send()
        exchange(backp, came, back_send, back_recv, t + 1).wait_send()

    loop(mp - 1, drain_exchange)


def write_out(*refs):
    sources, targets, sem = refs[:3], refs[3:6], refs[6]
    copies = [pltpu.make_async_copy(sources[i], targets[i], sem.at[i]) for i in range(3)]
    for copy in copies:
        copy.start()
    for copy in copies:
        copy.wait()


def per_device(n_dp, mp, grad_parts, left_stats, right_stats, left_root, right_root, owners):
    n = n_dp // CORES
    per, (rows, cols) = grad_parts.shape[1], grad_parts.shape[2:]
    held, slots = per // n_dp, left_stats.shape[2]
    hbm = pl.BlockSpec(memory_space=pltpu.HBM)

    def blocks(*lead, kind=BF16):
        return pltpu.VMEM((*lead, rows, cols), kind)

    dma = pltpu.SemaphoreType.DMA
    results = (
        pltpu.VMEM((per, rows, cols), BF16),
        pltpu.VMEM(left_stats.shape, F32),
        pltpu.VMEM(right_stats.shape, F32),
    )
    operands = [
        pltpu.with_memory_space_constraint(x, pltpu.HBM)
        for x in (owners, grad_parts, left_stats, right_stats, left_root, right_root)
    ]
    held_on_chip = pl.pallas_call(
        functools.partial(kernel, n, mp, held, slots),
        out_shape=results,
        in_specs=[hbm] * 6,
        out_specs=[pl.BlockSpec(memory_space=pltpu.VMEM)] * 3,
        scratch_shapes=[
            blocks(n * held), blocks(n * held), blocks(n * held), blocks(2, n * held),
            blocks(kind=F32), blocks(held), blocks(mp), blocks(mp), blocks(slots), blocks(slots),
            blocks(mp), blocks(mp), blocks(slots), blocks(slots),
            pltpu.SMEM(owners.shape, jnp.int32), pltpu.SMEM((mp,), jnp.int32),
            dma((n,)), dma((n,)), dma((n,)), dma((n * held,)), dma((2, n * held)),
            dma((mp,)), dma((mp,)), dma((mp,)), dma((mp,)),
            dma((2, n * held)), dma((n * held,)), dma((n * held,)), dma((n * held,)),
            dma((5,)), pltpu.SemaphoreType.REGULAR,
        ],
        compiler_params=pltpu.CompilerParams(
            collective_id=0, has_side_effects=True, vmem_limit_bytes=32 * 1024 * 1024),
    )(*operands)
    return pl.pallas_call(
        write_out,
        out_shape=[jax.ShapeDtypeStruct(x.shape, x.dtype) for x in held_on_chip],
        in_specs=[pl.BlockSpec(memory_space=pltpu.VMEM)] * 3,
        out_specs=[hbm] * 3,
        scratch_shapes=[dma((3,))],
        compiler_params=pltpu.CompilerParams(vmem_limit_bytes=1024 * 1024),
    )(*held_on_chip)


def solution(mesh):
    five = P("dp", "mp", None, None, None)
    return jax.shard_map(
        functools.partial(per_device, mesh.shape["dp"], mesh.shape["mp"]),
        mesh=mesh,
        in_specs=(P("dp", "mp", None, None), five, five, five, five, P()),
        out_specs=(P("mp", None, None), five, five),
        check_vma=False,
    )
```

```python
import functools

import jax
import jax.numpy as jnp
from jax import lax
from jax.experimental import pallas as pl
from jax.experimental.pallas import tpu as pltpu
from jax.sharding import PartitionSpec as P

CORES = 2
MESH = pl.DeviceIdType.MESH
F32, BF16 = jnp.float32, jnp.bfloat16


def kernel(
    n, mp, held, slots,
    owners_in, grads, left_in, right_in, lroot_in, rroot_in,
    dirbuf, lstat, rstat,
    own, part, partial, recv, accf, gbuf, pack, arrived, owned, prec, backp, came,
    lroot, rroot, owners, back_sel,
    own_sem, part_send, part_recv, red_send, red_recv, fwd_send, fwd_recv, back_send, back_recv,
    gat_send, gat_recv, pair_send, pair_recv, stat_sem, turn_sem,
):
    dp, me = lax.axis_index("dp"), lax.axis_index("mp")
    z, c = dp // CORES, dp % CORES
    partner = dp + 1 - 2 * c
    per = n * CORES * held

    def loop(count, body):
        def step(i, carry):
            body(i)
            return carry
        lax.fori_loop(0, count, step, 0)

    def own_copy(d):
        return pltpu.make_async_copy(
            grads.at[0, pl.ds((d * CORES + c) * held, held)],
            own.at[pl.ds(d * held, held)], own_sem.at[d])

    stat_copies = [
        pltpu.make_async_copy(lroot_in.at[0, 0], lroot, stat_sem.at[0]),
        pltpu.make_async_copy(rroot_in.at[0, 0], rroot, stat_sem.at[1]),
        pltpu.make_async_copy(left_in, lstat, stat_sem.at[2]),
        pltpu.make_async_copy(right_in, rstat, stat_sem.at[3]),
    ]
    owners_copy = pltpu.make_async_copy(owners_in, owners, stat_sem.at[4])
    owners_copy.start()
    loop(n, lambda d: own_copy(d).start())

    barrier = pltpu.get_barrier_semaphore()
    pl.semaphore_signal(barrier, inc=1, device_id={"dp": partner, "mp": me}, device_id_type=MESH)

    @pl.when(z > 0)
    def _():
        pl.semaphore_signal(barrier, inc=1, device_id={"dp": dp - CORES, "mp": me}, device_id_type=MESH)

    @pl.when(z < n - 1)
    def _():
        pl.semaphore_signal(barrier, inc=1, device_id={"dp": dp + CORES, "mp": me}, device_id_type=MESH)

    for k in range(1, mp):
        pl.semaphore_signal(
            barrier, inc=1, device_id={"dp": dp, "mp": lax.rem(me + k, mp)}, device_id_type=MESH)
    neighbours = jnp.where(z > 0, 1, 0) + jnp.where(z < n - 1, 1, 0)
    pl.semaphore_wait(barrier, mp + neighbours)

    def part_copy(d):
        return pltpu.make_async_remote_copy(
            src_ref=grads.at[0, pl.ds((d * CORES + 1 - c) * held, held)],
            dst_ref=part.at[pl.ds(d * held, held)],
            send_sem=part_send.at[d], recv_sem=part_recv.at[d],
            device_id={"dp": partner, "mp": me}, device_id_type=MESH)

    toward = jnp.where(2 * z < n, 1, -1)

    def far_first(t, sign):
        return jnp.where(sign > 0, n - 1 - t, t)

    loop(n, lambda t: part_copy(far_first(t, toward)).start())
    for copy in stat_copies:
        copy.start()

    def red_copy(d, j, sign, lane):
        i = d * held + j
        return pltpu.make_async_remote_copy(
            src_ref=partial.at[i], dst_ref=recv.at[lane, i],
            send_sem=red_send.at[i], recv_sem=red_recv.at[lane, i],
            device_id={"dp": dp + CORES * sign, "mp": me}, device_id_type=MESH)

    def both(d):
        own_copy(d).wait()
        part_copy(d).wait_recv()

    def red_step(t):
        for stream in range(2):
            sign = toward if stream == 0 else -toward
            lane = jnp.where(sign > 0, 0, 1)
            d = far_first(t, sign)
            before = z - sign

            @pl.when((d - z) * sign > 0)
            def _():
                both(d)

                def block(j):
                    i = d * held + j
                    has = (before >= 0) & (before < n)

                    @pl.when(has)
                    def _():
                        red_copy(d, j, sign, lane).wait_recv()
                        partial[i] = (
                            own[i].astype(F32) + part[i].astype(F32) + recv[lane, i].astype(F32)
                        ).astype(BF16)

                    @pl.when(jnp.logical_not(has))
                    def _():
                        partial[i] = (own[i].astype(F32) + part[i].astype(F32)).astype(BF16)

                    red_copy(d, j, sign, lane).start()

                loop(held, block)

    @pl.when(c == 1)
    def _():
        pl.semaphore_wait(turn_sem, 1)

    loop(n - 1, red_step)

    def last_sum(d, j):
        return (d == z + toward) & (j == held - 1)

    def sums_left(d):
        @pl.when(d != z)
        def _():
            def block(j):
                @pl.when(jnp.logical_not(last_sum(d, j)))
                def _():
                    red_copy(d, j, 1, 0).wait_send()

            loop(held, block)

    @pl.when(c == 0)
    def _():
        loop(n, sums_left)
        pl.semaphore_signal(
            turn_sem, inc=1, device_id={"dp": partner, "mp": me}, device_id_type=MESH)

    owners_copy.wait()
    my_owner = [owners[me * per + dp * held + j] for j in range(held)]

    def held_for(q):
        pick = jnp.int32(0)
        for j in range(held):
            pick = jnp.where(my_owner[j] == q, j, pick)
        return pick

    count = jnp.int32(0)
    source = [jnp.int32(0)] * slots
    filled = [jnp.int32(0)] * slots
    for q in range(mp):
        slot_for_q = jnp.int32(0)
        for j in range(held):
            mine = owners[q * per + dp * held + j] == me
            for s in range(slots):
                hit = mine & (count == s)
                source[s] = jnp.where(hit, q, source[s])
                filled[s] = jnp.where(hit, 1, filled[s])
                slot_for_q = jnp.where(hit, s, slot_for_q)
            count = count + mine.astype(jnp.int32)
        back_sel[q] = slot_for_q

    both(z)

    def finish(j):
        i = z * held + j
        accf[...] = own[i].astype(F32) + part[i].astype(F32)

        @pl.when(z > 0)
        def _():
            red_copy(z, j, 1, 0).wait_recv()
            accf[...] += recv[0, i].astype(F32)

        @pl.when(z < n - 1)
        def _():
            red_copy(z, j, -1, 1).wait_recv()
            accf[...] += recv[1, i].astype(F32)

        gbuf[j] = accf[...].astype(BF16)

    loop(held, finish)

    def exchange(src, dst, sends, recvs, k):
        return pltpu.make_async_remote_copy(
            src_ref=src.at[k], dst_ref=dst.at[me],
            send_sem=sends.at[k], recv_sem=recvs.at[k],
            device_id={"dp": dp, "mp": lax.rem(me + k, mp)}, device_id_type=MESH)

    def send_held(t):
        k = mp - 1 - t
        pack[k] = gbuf[held_for(lax.rem(me + k, mp))]
        exchange(pack, arrived, fwd_send, fwd_recv, k).start()

    loop(mp - 1, send_held)
    arrived[me] = gbuf[held_for(me)]
    for copy in stat_copies[:2]:
        copy.wait()
    loop(mp - 1, lambda t: exchange(pack, arrived, fwd_send, fwd_recv, t + 1).wait_recv())

    def dot(a, b, dims=((1,), (0,))):
        return lax.dot_general(a, b, (dims, ((), ())), preferred_element_type=F32)

    for s in range(slots):
        block = arrived[source[s]]
        owned[s] = jnp.where(filled[s] > 0, block.astype(F32), 0.0).astype(BF16)
    halves = [dot(lroot[s], owned[s]).astype(BF16) for s in range(slots)]
    steps = [dot(halves[s], rroot[s]).astype(BF16) for s in range(slots)]
    for s in range(slots):
        prec[s] = steps[s]

    def send_back(t):
        k = mp - 1 - t
        backp[k] = prec[back_sel[lax.rem(me + k, mp)]]
        exchange(backp, came, back_send, back_recv, k).start()

    loop(mp - 1, send_back)
    came[me] = prec[back_sel[me]]

    for copy in stat_copies[2:]:
        copy.wait()
    for s in range(slots):
        lstat[0, 0, s] += dot(owned[s], owned[s], ((1,), (1,)))
    loop(mp - 1, lambda t: exchange(backp, came, back_send, back_recv, t + 1).wait_recv())
    for j in range(held):
        dirbuf[dp * held + j] = came[my_owner[j]]

    def gat_copy(r, j, sign, lane):
        i = (r * CORES + c) * held + j
        return pltpu.make_async_remote_copy(
            src_ref=dirbuf.at[i], dst_ref=dirbuf.at[i],
            send_sem=gat_send.at[lane, r * held + j], recv_sem=gat_recv.at[r * held + j],
            device_id={"dp": dp + CORES * sign, "mp": me}, device_id_type=MESH)

    def pair_copy(r, j, core):
        i = (r * CORES + core) * held + j
        return pltpu.make_async_remote_copy(
            src_ref=dirbuf.at[i], dst_ref=dirbuf.at[i],
            send_sem=pair_send.at[r * held + j], recv_sem=pair_recv.at[r * held + j],
            device_id={"dp": partner, "mp": me}, device_id_type=MESH)

    def first(j):
        @pl.when(z < n - 1)
        def _():
            gat_copy(z, j, 1, 0).start()

        @pl.when(z > 0)
        def _():
            gat_copy(z, j, -1, 1).start()

        pair_copy(z, j, c).start()

    loop(held, first)
    for s in range(slots):
        rstat[0, 0, s] += dot(owned[s], owned[s], ((0,), (0,)))

    def gather_step(t):
        for lane, sign in ((0, 1), (1, -1)):
            r = z - sign * (t + 1)
            after = z + sign

            @pl.when((r >= 0) & (r < n))
            def _():
                def block(j):
                    gat_copy(r, j, sign, lane).wait_recv()

                    @pl.when((after >= 0) & (after < n))
                    def _():
                        gat_copy(r, j, sign, lane).start()

                    pair_copy(r, j, c).start()

                loop(held, block)

    loop(n - 1, gather_step)

    def pair_row(r):
        loop(held, lambda j: pair_copy(r, j, 1 - c).wait_recv())

    pair_row(z)

    def pair_step(t):
        for sign in (1, -1):
            r = z - sign * (t + 1)

            @pl.when((r >= 0) & (r < n))
            def _():
                pair_row(r)

    loop(n - 1, pair_step)

    def drain(r):
        part_copy(r).wait_send()

        def block(j):
            pair_copy(r, j, c).wait_send()

            @pl.when((r != z) & ((c == 1) | last_sum(r, j)))
            def _():
                red_copy(r, j, 1, 0).wait_send()

            @pl.when((r <= z) & (z < n - 1))
            def _():
                gat_copy(r, j, 1, 0).wait_send()

            @pl.when((r >= z) & (z > 0))
            def _():
                gat_copy(r, j, -1, 1).wait_send()

        loop(held, block)

    loop(n, drain)

    def drain_exchange(t):
        exchange(pack, arrived, fwd_send, fwd_recv, t + 1).wait_send()
        exchange(backp, came, back_send, back_recv, t + 1).wait_send()

    loop(mp - 1, drain_exchange)


def write_out(*refs):
    sources, targets, sem = refs[:3], refs[3:6], refs[6]
    copies = [pltpu.make_async_copy(sources[i], targets[i], sem.at[i]) for i in range(3)]
    for copy in copies:
        copy.start()
    for copy in copies:
        copy.wait()


def per_device(n_dp, mp, grad_parts, left_stats, right_stats, left_root, right_root, owners):
    n = n_dp // CORES
    per, (rows, cols) = grad_parts.shape[1], grad_parts.shape[2:]
    held, slots = per // n_dp, left_stats.shape[2]
    hbm = pl.BlockSpec(memory_space=pltpu.HBM)

    def blocks(*lead, kind=BF16):
        return pltpu.VMEM((*lead, rows, cols), kind)

    dma = pltpu.SemaphoreType.DMA
    results = (
        pltpu.VMEM((per, rows, cols), BF16),
        pltpu.VMEM(left_stats.shape, F32),
        pltpu.VMEM(right_stats.shape, F32),
    )
    operands = [
        pltpu.with_memory_space_constraint(x, pltpu.HBM)
        for x in (owners, grad_parts, left_stats, right_stats, left_root, right_root)
    ]
    held_on_chip = pl.pallas_call(
        functools.partial(kernel, n, mp, held, slots),
        out_shape=results,
        in_specs=[hbm] * 6,
        out_specs=[pl.BlockSpec(memory_space=pltpu.VMEM)] * 3,
        scratch_shapes=[
            blocks(n * held), blocks(n * held), blocks(n * held), blocks(2, n * held),
            blocks(kind=F32), blocks(held), blocks(mp), blocks(mp), blocks(slots), blocks(slots),
            blocks(mp), blocks(mp), blocks(slots), blocks(slots),
            pltpu.SMEM(owners.shape, jnp.int32), pltpu.SMEM((mp,), jnp.int32),
            dma((n,)), dma((n,)), dma((n,)), dma((n * held,)), dma((2, n * held)),
            dma((mp,)), dma((mp,)), dma((mp,)), dma((mp,)),
            dma((2, n * held)), dma((n * held,)), dma((n * held,)), dma((n * held,)),
            dma((5,)), pltpu.SemaphoreType.REGULAR,
        ],
        compiler_params=pltpu.CompilerParams(
            collective_id=0, has_side_effects=True, vmem_limit_bytes=32 * 1024 * 1024),
    )(*operands)
    return pl.pallas_call(
        write_out,
        out_shape=[jax.ShapeDtypeStruct(x.shape, x.dtype) for x in held_on_chip],
        in_specs=[pl.BlockSpec(memory_space=pltpu.VMEM)] * 3,
        out_specs=[hbm] * 3,
        scratch_shapes=[dma((3,))],
        compiler_params=pltpu.CompilerParams(vmem_limit_bytes=1024 * 1024),
    )(*held_on_chip)


def solution(mesh):
    five = P("dp", "mp", None, None, None)
    return jax.shard_map(
        functools.partial(per_device, mesh.shape["dp"], mesh.shape["mp"]),
        mesh=mesh,
        in_specs=(P("dp", "mp", None, None), five, five, five, five, P()),
        out_specs=(P("mp", None, None), five, five),
        check_vma=False,
    )
```
